32 devices in a mesh: section: 4 (over y, x), seq: 8 (over z, core).
Axes of the slice: x: 2, y: 2, z: 4, core: 2. Of those that a mesh axis runs over, the one named last changes fastest.
Arguments:
- queries: bfloat16 [4, 1024, 4096], P('section', 'seq'), may hold values from -500 to 500
- keys: bfloat16 [4, 1024, 512], P('section', 'seq'), may hold values from -6 to 6
- values: bfloat16 [4, 1024, 512], P('section', 'seq'), may hold values from -6 to 6
- out_grad: bfloat16 [4, 1024, 4096], P('section', 'seq'), may hold values from -6 to 6
- documents: int32 [4, 1024], P('section'), may hold values from 0 to 3, never falling along the last dimension, each value on 1 to 512 neighbouring positions
- query_weight: bfloat16 [4, 4096, 4096], P('section', 'seq'), may hold values from -0.09375 to 0.09375
- key_weight: bfloat16 [4, 512, 4096], P('section'), may hold values from -0.1875 to 0.1875
- value_weight: bfloat16 [4, 512, 4096], P('section'), may hold values from -0.1875 to 0.1875
Outputs:
- upstream: bfloat16 [4, 1024, 4096], P('section', 'seq')
The draws below stay inside these ranges and needn't reach their ends.
Inputs may be any that keep to these rules, and one draw needn't show every extreme that they name: `documents`: each section's document ids never fall along its tokens.
All inputs are finite; a program needn't handle non-finite values.
Results may differ from the reference program's by a relative error of at most 0.0058.
Values may be sent and summed in bfloat16 or wider, within the bound.
A program may use at most 192 MiB of HBM per device.

```python
import math
import jax
import jax.numpy as jnp
import numpy as np
from jax import lax

D = 4096
H = 32
KV = 4
HD = 128
SECTIONS = 4
TOKENS = 1024
N_SEQ = 8


def query_key_pair(key):
    base = jax.random.fold_in(key, 11)
    key_q, key_k = jax.random.split(base, 2)
    queries = jax.random.normal(key_q, (SECTIONS, TOKENS, H * HD), jnp.float32)
    keys = jax.random.normal(key_k, (SECTIONS, TOKENS, KV * HD), jnp.float32)
    keys = jnp.clip(keys, -6.0, 6.0)
    return (queries, keys)


def draw_queries(key, part):
    return query_key_pair(key)[0].astype(jnp.bfloat16)


def draw_keys(key, part):
    return query_key_pair(key)[1].astype(jnp.bfloat16)


def shard_levels(rng, shape, shards, least, top_value):
    def one(axis_at, parts):
        draws = jax.random.uniform(jax.random.fold_in(jax.random.fold_in(rng, 6), axis_at), (parts,), jnp.float32, least / len(shards), top_value / len(shards))
        return jnp.repeat(jnp.exp(draws), shape[axis_at] // parts).reshape((-1,) + (1,) * (len(shape) - axis_at - 1))

    loudness = one(*shards[0])
    for cut in shards[1:]:
        loudness = loudness * one(*cut)
    return loudness


def split_up(amount, total, most, slope):
    weights = [(1 << 20) // math.isqrt(rank ** slope) + 1 for rank in range(2, amount + 1)]
    rest, counts = total - most - (amount - 1), [1] * (amount - 1)
    while rest > 0:
        movable = [i for i in range(amount - 1) if counts[i] < most]
        pool, remaining = sum([weights[i] for i in movable]), rest
        for i in movable:
            extra = min(most - counts[i], max(1, remaining * weights[i] // pool), rest)
            counts[i] = counts[i] + extra
            rest = rest - extra
    return np.array([most] + counts)


def ragged(own_key, amount, total, bound, slope):
    if amount == 2:
        one = jax.random.randint(own_key, (), max(1, total - bound), min(bound, total - 1) + 1)
        return jnp.stack([one, total - one])
    tallies = jnp.asarray(split_up(amount, total, bound, slope), jnp.int32)
    twos = (amount - 1) // 2
    donor, taker = tallies[1:1 + 2 * twos:2], tallies[2:2 + 2 * twos:2]
    slack = jnp.minimum(donor - 1, bound - taker)
    passed = jax.random.randint(jax.random.fold_in(own_key, 1), (twos,), 0, 1 << 20) % (slack + 1)
    tallies = tallies.at[1:1 + 2 * twos:2].set(donor - passed).at[2:2 + 2 * twos:2].set(taker + passed)
    return tallies[jax.random.permutation(jax.random.fold_in(own_key, 2), amount)]


def normal_values(key, dims, deviation, reach, cuts=(), kind=jnp.bfloat16):
    loudness = shard_levels(key, dims, cuts, -0.22, 0.18) if cuts else 1.0
    array = jax.random.normal(key, dims, jnp.float32) * deviation * loudness
    return jnp.minimum(jnp.maximum(array, -reach), reach).astype(kind)


def setup_inputs(seed: int = 0) -> dict:
    streams_of = jax.random.split(jax.random.key(seed), 9)
    return {
        "queries": draw_queries(jax.random.fold_in(streams_of[8], 71), 0),
        "keys": draw_keys(jax.random.fold_in(streams_of[8], 71), 0),
        "values": normal_values(streams_of[2], (SECTIONS, TOKENS, KV * HD), 1.0, 6.0, ((0, 4), (1, 8))),
        "out_grad": normal_values(streams_of[3], (SECTIONS, TOKENS, H * HD), 1.0, 6.0, ((0, 4), (1, 8))),
        "documents": jax.vmap(lambda own: jnp.searchsorted(jnp.cumsum(ragged(own, 4, TOKENS, TOKENS // 2, 0)), jnp.arange(TOKENS), side="right"))(jax.random.split(streams_of[4], SECTIONS)).reshape((SECTIONS, TOKENS)).astype(jnp.int32),
        "query_weight": normal_values(streams_of[5], (SECTIONS, H * HD, D), (H * HD) ** -0.5, 0.09375, ((0, 4), (1, 8))),
        "key_weight": normal_values(streams_of[6], (SECTIONS, KV * HD, D), (N_SEQ * HD) ** -0.5, 0.1875, ((0, 4),)),
        "value_weight": normal_values(streams_of[7], (SECTIONS, KV * HD, D), (N_SEQ * HD) ** -0.5, 0.1875, ((0, 4),)),
    }


def slot_grads(index, q_all, k_all, v_all, o_all, ids):
    per = H // N_SEQ
    total = q_all.shape[0]
    kvh = index * KV // N_SEQ
    scale = 1.0 / math.sqrt(HD)
    q_blk = lax.dynamic_slice_in_dim(q_all, index * per * HD, per * HD, 1).reshape(total, per, HD).astype(jnp.float32)
    o_blk = lax.dynamic_slice_in_dim(o_all, index * per * HD, per * HD, 1).reshape(total, per, HD).astype(jnp.float32)
    k_head = lax.dynamic_slice_in_dim(k_all, kvh * HD, HD, 1).astype(jnp.float32)
    v_head = lax.dynamic_slice_in_dim(v_all, kvh * HD, HD, 1).astype(jnp.float32)
    rows = lax.iota(jnp.int32, total)
    allowed = (rows[None, :] <= rows[:, None]) & (ids[None, :] == ids[:, None])
    scores = jnp.einsum('bhd,td->hbt', q_blk, k_head) * scale
    scores = jnp.where(allowed[None], scores, -jnp.inf)
    top = lax.optimization_barrier(jnp.max(scores, axis=-1, keepdims=True))
    expo = jnp.exp(scores - top)
    prob = expo / lax.optimization_barrier(jnp.sum(expo, axis=-1, keepdims=True))
    prob_low = prob.astype(jnp.bfloat16)
    dprob = jnp.einsum('bhd,td->hbt', o_blk, v_head)
    delta = lax.optimization_barrier(jnp.sum(prob * dprob, axis=-1, keepdims=True))
    dscore = (prob * (dprob - delta) * scale).astype(jnp.bfloat16).astype(jnp.float32)
    dquery = jnp.einsum('hbt,td->bhd', dscore, k_head).astype(jnp.bfloat16).reshape(total, per * HD)
    dkey = jnp.einsum('hbt,bhd->td', dscore, q_blk).astype(jnp.bfloat16)
    dvalue = jnp.einsum('hbt,bhd->td', prob_low.astype(jnp.float32), o_blk).astype(jnp.bfloat16)
    return (dquery, dkey, dvalue)

def reference(queries, keys, values, out_grad, documents, query_weight, key_weight, value_weight):
    reps = N_SEQ // KV
    grads = []
    for section in range(SECTIONS):

        def one_slot(index):
            return slot_grads(index, queries[section], keys[section], values[section], out_grad[section], documents[section])
        dq_s, dk_s, dv_s = lax.map(one_slot, jnp.arange(N_SEQ, dtype=jnp.int32))
        total = queries.shape[1]
        dquery = jnp.transpose(dq_s, (1, 0, 2)).reshape(total, H * HD)
        dkey = jnp.transpose(dk_s, (1, 0, 2)).reshape(total, N_SEQ * HD)
        dvalue = jnp.transpose(dv_s, (1, 0, 2)).reshape(total, N_SEQ * HD)
        wk_rep = jnp.repeat(key_weight[section].reshape(KV, HD, D), reps, axis=0).reshape(N_SEQ * HD, D)
        wv_rep = jnp.repeat(value_weight[section].reshape(KV, HD, D), reps, axis=0).reshape(N_SEQ * HD, D)
        dinput = jnp.dot(dquery, query_weight[section], preferred_element_type=jnp.float32)
        dinput = dinput + jnp.dot(dkey, wk_rep, preferred_element_type=jnp.float32)
        dinput = dinput + jnp.dot(dvalue, wv_rep, preferred_element_type=jnp.float32)
        grads.append(dinput.astype(jnp.bfloat16))
    grads = grads[1:] + [jnp.zeros_like(grads[0])]
    return jnp.stack(grads, axis=0)
```

```python
import functools
import math

import jax
import jax.numpy as jnp
from jax import lax
from jax.experimental import pallas as pl
from jax.experimental.pallas import tpu as pltpu
from jax.sharding import PartitionSpec as P

KV = 4
HD = 128
MESH = pl.DeviceIdType.MESH
F32 = jnp.float32
BF16 = jnp.bfloat16


def aligned(index, size):
    return pl.ds(pl.multiple_of(index * size, size), size)


def kernel(dims, q_in, k_in, v_in, o_in, start_ref, wq_in, wk_in, wv_in, out_ref,
           q_all, o_all, k_all, v_all, k_turned, dk_sum, dv_sum, grads, weights,
           right_buf, left_buf, acc, final,
           q_sent, o_sent, k_sent, v_sent, q_got, o_got, kv_got,
           w_local, w_sent, w_got, g_sent, g_got,
           right_sent, right_got, left_sent, left_got, final_sent, final_got):
    sections, count, tok, heads, width, block, cw = dims
    total = tok * count
    chips = count // 2
    rows = 2 * tok
    feats = heads * HD
    half = width // 2
    chunks = half // cw
    scale = 1.0 / math.sqrt(HD)
    to_log2 = scale * math.log2(math.e)
    sec = lax.axis_index("section")
    me = lax.axis_index("seq")
    chip = me // 2
    core = me % 2
    partner = (sec, me + 1 - 2 * core)

    barrier = pltpu.get_barrier_semaphore()

    def greet(device):
        pl.semaphore_signal(barrier, inc=1, device_id=device, device_id_type=MESH)

    for off in range(1, count):
        greet((sec, lax.rem(me + off, count)))
    for p in range(2):
        @pl.when(sec > 0)
        def _():
            greet((sec - 1, 2 * chip + p))

        @pl.when(sec < sections - 1)
        def _():
            greet((sec + 1, 2 * chip + p))
    above = jnp.where(sec > 0, 2, 0)
    below = jnp.where(sec < sections - 1, 2, 0)
    pl.semaphore_wait(barrier, count - 1 + above + below)

    def remote(src, dst, send_sem, recv_sem, device):
        return pltpu.make_async_remote_copy(
            src_ref=src, dst_ref=dst, send_sem=send_sem, recv_sem=recv_sem,
            device_id=device, device_id_type=MESH)

    def kv_copy(off, which):
        peer = lax.rem(me + off, count)
        src, dst, sem = ((k_in, k_all, k_sent), (v_in, v_all, v_sent))[which]
        return remote(src.at[:, aligned(peer * KV // count, HD)], dst.at[aligned(me, tok)],
                      sem.at[off], kv_got.at[which], (sec, peer))

    def qo_copy(off, h, which):
        peer = lax.rem(me + off, count)
        src, dst, sem, got = ((q_in, q_all, q_sent, q_got), (o_in, o_all, o_sent, o_got))[which]
        return remote(src.at[:, aligned(peer * heads + h, HD)], dst.at[h, aligned(me, tok)],
                      sem.at[h, off], got.at[h], (sec, peer))

    def w_copy():
        return remote(wq_in.at[:, aligned(1 - core, half)], weights.at[aligned(core, feats)],
                      w_sent.at[0], w_got.at[0], partner)

    for off in range(1, count):
        kv_copy(off, 0).start()
        kv_copy(off, 1).start()

    def send_head(h, carry):
        for off in range(1, count):
            qo_copy(off, h, 0).start()
            qo_copy(off, h, 1).start()
        return carry

    lax.fori_loop(0, heads, send_head, 0)
    w_copy().start()

    mine = aligned(me, tok)
    own = aligned(me * KV // count, HD)
    pltpu.make_async_copy(k_in.at[:, own], k_all.at[mine], kv_got.at[0]).start()
    pltpu.make_async_copy(v_in.at[:, own], v_all.at[mine], kv_got.at[1]).start()

    def own_head(h, carry):
        cols = aligned(me * heads + h, HD)
        pltpu.make_async_copy(q_in.at[:, cols], q_all.at[h, mine], q_got.at[h]).start()
        pltpu.make_async_copy(o_in.at[:, cols], o_all.at[h, mine], o_got.at[h]).start()
        return carry

    lax.fori_loop(0, heads, own_head, 0)

    my_half = aligned(core, half)
    local = [pltpu.make_async_copy(wq_in.at[:, my_half], weights.at[aligned(core, feats)],
                                   w_local.at[0])]
    for p in range(2):
        g = aligned((2 * chip + p) * KV // count, HD)
        base = 2 * feats + p * HD
        local.append(pltpu.make_async_copy(
            wk_in.at[g, my_half], weights.at[base:base + HD], w_local.at[1 + p]))
        local.append(pltpu.make_async_copy(
            wv_in.at[g, my_half], weights.at[base + 2 * HD:base + 3 * HD], w_local.at[3 + p]))
    for copy in local:
        copy.start()

    @pl.when(sec == sections - 1)
    def _():
        out_ref[...] = jnp.zeros_like(out_ref)

    dk_sum[...] = jnp.zeros_like(dk_sum)
    dv_sum[...] = jnp.zeros_like(dv_sum)

    pltpu.make_async_copy(k_all, k_all, kv_got.at[0]).wait()
    pltpu.make_async_copy(v_all, v_all, kv_got.at[1]).wait()
    k_turned[...] = k_all[...].T

    def grad_copy(col, index):
        here = grads.at[:, col]
        return remote(here, here, g_sent.at[index], g_got.at[index], partner)

    def head_cols(p, h):
        return aligned(p * heads + h, HD)

    def tail_cols(p, which):
        return aligned(2 * heads + 2 * which + p, HD)

    def attend(h, carry):
        pltpu.make_async_copy(q_all.at[h], q_all.at[h], q_got.at[h]).wait()
        pltpu.make_async_copy(o_all.at[h], o_all.at[h], o_got.at[h]).wait()
        cols = head_cols(core, h)
        for i in range(total // block):
            lo, hi = i * block, (i + 1) * block
            q = q_all[h, lo:hi, :]
            o = o_all[h, lo:hi, :]
            last = (((1,), (1,)), ((), ()))
            s = lax.dot_general(k_all[:hi], q, last, preferred_element_type=F32)
            dp = lax.dot_general(v_all[:hi], o, last, preferred_element_type=F32)
            j = lax.broadcasted_iota(jnp.int32, (hi, block), 0)
            at = lax.broadcasted_iota(jnp.int32, (hi, block), 1) + lo
            allowed = (j >= start_ref[:, lo:hi]) & (j <= at)
            s = jnp.where(allowed, s, -jnp.inf)
            top = jnp.max(s, axis=0, keepdims=True)
            e = jnp.exp2((s - top) * to_log2)
            inv = 1.0 / jnp.sum(e, axis=0, keepdims=True)
            delta = jnp.sum(e * dp, axis=0, keepdims=True) * inv
            p_low = (e * inv).astype(BF16)
            ds = (e * (dp - delta) * (inv * scale)).astype(BF16)
            dv_sum[:hi] += jnp.dot(p_low, o, preferred_element_type=F32)
            dk_sum[:hi] += jnp.dot(ds, q, preferred_element_type=F32)
            dq = jnp.dot(k_turned[:, :hi], ds, preferred_element_type=F32)
            grads[lo:hi, cols] = dq.T.astype(BF16)
        grad_copy(cols, h).start()
        return carry

    lax.fori_loop(0, heads, attend, 0)
    grads[:, tail_cols(core, 0)] = dk_sum[...].astype(BF16)
    grads[:, tail_cols(core, 1)] = dv_sum[...].astype(BF16)
    for which in range(2):
        grad_copy(tail_cols(core, which), heads + which).start()
    for copy in local:
        copy.wait()
    remote(wq_in.at[:, my_half], weights.at[aligned(1 - core, feats)],
           w_sent.at[0], w_got.at[0], partner).wait_recv()
    for h in range(heads):
        grad_copy(head_cols(1 - core, h), h).wait_recv()
    for which in range(2):
        grad_copy(tail_cols(1 - core, which), heads + which).wait_recv()

    def right_copy(d, k):
        here = right_buf.at[d, k]
        return remote(here, here, right_sent.at[d, k], right_got.at[d, k],
                      (sec, jnp.minimum(me + 2, count - 2 + core)))

    def left_copy(d, k):
        here = left_buf.at[d, k]
        return remote(here, here, left_sent.at[d, k], left_got.at[d, k],
                      (sec, jnp.maximum(me - 2, core)))

    def final_copy(k, p):
        return remote(final.at[k, p * tok:(p + 1) * tok],
                      out_ref.at[:, aligned(core * chunks + k, cw)],
                      final_sent.at[k, p], final_got.at[core, k],
                      (jnp.maximum(sec - 1, 0), 2 * chip + p))

    def product(d, k):
        return jnp.dot(grads[aligned(d, rows), :], weights[:, aligned(k, cw)],
                       preferred_element_type=F32)

    def pass_on(d, k, buf, copy, first):
        acc[...] = product(d, k)

        @pl.when(jnp.logical_not(first))
        def _():
            copy(d, k).wait_recv()
            buf[d, k] = (acc[...] + buf[d, k].astype(F32)).astype(BF16)

        @pl.when(first)
        def _():
            buf[d, k] = acc[...].astype(BF16)

        copy(d, k).start()

    def finish(k):
        acc[...] = product(chip, k)

        @pl.when(chip > 0)
        def _():
            right_copy(chip, k).wait_recv()
            acc[...] += right_buf[chip, k].astype(F32)

        @pl.when(chip < chips - 1)
        def _():
            left_copy(chip, k).wait_recv()
            acc[...] += left_buf[chip, k].astype(F32)

        final[k] = acc[...].astype(BF16)

        @pl.when(sec > 0)
        def _():
            final_copy(k, 0).start()
            final_copy(k, 1).start()

    lag = min(2, chunks)

    def step(k, carry):
        @pl.when(k < chunks)
        def _():
            def to_right(i, c):
                pass_on(chips - 1 - i, k, right_buf, right_copy, chip == 0)
                return c

            def to_left(i, c):
                pass_on(i, k, left_buf, left_copy, chip == chips - 1)
                return c

            lax.fori_loop(0, chips - 1 - chip, to_right, 0)
            lax.fori_loop(0, chip, to_left, 0)

        @pl.when(k >= lag)
        def _():
            finish(k - lag)

        return carry

    lax.fori_loop(0, chunks + lag, step, 0)

    for off in range(1, count):
        kv_copy(off, 0).wait_send()
        kv_copy(off, 1).wait_send()

    def sent_head(h, carry):
        for off in range(1, count):
            qo_copy(off, h, 0).wait_send()
            qo_copy(off, h, 1).wait_send()
        grad_copy(head_cols(core, h), h).wait_send()
        return carry

    lax.fori_loop(0, heads, sent_head, 0)
    for which in range(2):
        grad_copy(tail_cols(core, which), heads + which).wait_send()
    w_copy().wait_send()

    def drain(k, carry):
        def right_done(i, c):
            right_copy(chips - 1 - i, k).wait_send()
            return c

        def left_done(i, c):
            left_copy(i, k).wait_send()
            return c

        lax.fori_loop(0, chips - 1 - chip, right_done, 0)
        lax.fori_loop(0, chip, left_done, 0)

        @pl.when(sec > 0)
        def _():
            final_copy(k, 0).wait_send()
            final_copy(k, 1).wait_send()

        @pl.when(sec < sections - 1)
        def _():
            for p in range(2):
                remote(final.at[k, :tok], out_ref.at[:, aligned(p * chunks + k, cw)],
                       final_sent.at[k, p], final_got.at[p, k], partner).wait_recv()

        return carry

    lax.fori_loop(0, chunks, drain, 0)


def body(queries, keys, values, out_grad, documents, query_weight, key_weight, value_weight):
    sections = lax.axis_size("section")
    count = lax.axis_size("seq")
    tok = queries.shape[1]
    total = tok * count
    feats = query_weight.shape[1]
    heads = feats // HD
    width = query_weight.shape[2]
    chips = count // 2
    rows = 2 * tok
    block = min(256, total)
    cw = min(256, width // 2)
    chunks = width // 2 // cw
    ids = documents[0]
    start = jnp.sum((ids[:, None] < ids[None, :]).astype(jnp.int32), axis=0, keepdims=True)
    dma = pltpu.SemaphoreType.DMA
    deep = 2 * feats + 4 * HD
    anywhere = pl.BlockSpec(memory_space=pl.ANY)
    vmem = pl.BlockSpec(memory_space=pltpu.VMEM)
    out = pl.pallas_call(
        functools.partial(kernel, (sections, count, tok, heads, width, block, cw)),
        out_shape=jax.ShapeDtypeStruct((tok, width), BF16),
        in_specs=[anywhere] * 4 + [vmem] + [anywhere] * 3,
        out_specs=vmem,
        scratch_shapes=[
            pltpu.VMEM((heads, total, HD), BF16),
            pltpu.VMEM((heads, total, HD), BF16),
            pltpu.VMEM((total, HD), BF16),
            pltpu.VMEM((total, HD), BF16),
            pltpu.VMEM((HD, total), BF16),
            pltpu.VMEM((total, HD), F32),
            pltpu.VMEM((total, HD), F32),
            pltpu.VMEM((total, deep), BF16),
            pltpu.VMEM((deep, width // 2), BF16),
            pltpu.VMEM((chips, chunks, rows, cw), BF16),
            pltpu.VMEM((chips, chunks, rows, cw), BF16),
            pltpu.VMEM((rows, cw), F32),
            pltpu.VMEM((chunks, rows, cw), BF16),
            dma((heads, count)),
            dma((heads, count)),
            dma((count,)),
            dma((count,)),
            dma((heads,)),
            dma((heads,)),
            dma((2,)),
            dma((5,)),
            dma((1,)),
            dma((1,)),
            dma((heads + 2,)),
            dma((heads + 2,)),
            dma((chips, chunks)),
            dma((chips, chunks)),
            dma((chips, chunks)),
            dma((chips, chunks)),
            dma((chunks, 2)),
            dma((2, chunks)),
        ],
        compiler_params=pltpu.CompilerParams(
            collective_id=0, has_side_effects=True, vmem_limit_bytes=62 * 1024 * 1024),
        name="attention_back",
    )(queries[0], keys[0], values[0], out_grad[0], start,
      query_weight[0], key_weight[0], value_weight[0])
    return out[None]


def solution(mesh):
    in_specs = (
        P("section", "seq", None),
        P("section", "seq", None),
        P("section", "seq", None),
        P("section", "seq", None),
        P("section", None),
        P("section", "seq", None),
        P("section", None, None),
        P("section", None, None),
    )
    out_specs = P("section", "seq", None)
    return jax.shard_map(body, mesh=mesh, in_specs=in_specs, out_specs=out_specs, check_vma=False)
```

```python
import functools
import math

import jax
import jax.numpy as jnp
from jax import lax
from jax.experimental import pallas as pl
from jax.experimental.pallas import tpu as pltpu
from jax.sharding import PartitionSpec as P

KV = 4
HD = 128
MESH = pl.DeviceIdType.MESH
F32 = jnp.float32
BF16 = jnp.bfloat16


def aligned(index, size):
    return pl.ds(pl.multiple_of(index * size, size), size)


def kernel(dims, q_in, k_in, v_in, o_in, start_ref, wq_in, wk_in, wv_in, out_ref,
           q_all, o_all, k_all, v_all, k_turned, dk_sum, dv_sum, grads, weights,
           right_buf, left_buf, acc, final,
           q_sent, o_sent, k_sent, v_sent, q_got, o_got, kv_got,
           w_local, w_sent, w_got, g_sent, g_got,
           right_sent, right_got, left_sent, left_got, final_sent, final_got):
    sections, count, tok, heads, width, cw = dims
    total = tok * count
    chips = count // 2
    rows = 2 * tok
    feats = heads * HD
    span = feats + 2 * HD
    half = width // 2
    chunks = half // cw
    scale = 1.0 / math.sqrt(HD)
    to_log2 = scale * math.log2(math.e)
    sec = lax.axis_index("section")
    me = lax.axis_index("seq")
    chip = me // 2
    core = me % 2
    partner = (sec, me + 1 - 2 * core)

    barrier = pltpu.get_barrier_semaphore()

    def greet(device):
        pl.semaphore_signal(barrier, inc=1, device_id=device, device_id_type=MESH)

    for off in range(1, count):
        greet((sec, lax.rem(me + off, count)))
    for p in range(2):
        @pl.when(sec > 0)
        def _():
            greet((sec - 1, 2 * chip + p))

        @pl.when(sec < sections - 1)
        def _():
            greet((sec + 1, 2 * chip + p))
    above = jnp.where(sec > 0, 2, 0)
    below = jnp.where(sec < sections - 1, 2, 0)
    pl.semaphore_wait(barrier, count - 1 + above + below)

    def remote(src, dst, send_sem, recv_sem, device):
        return pltpu.make_async_remote_copy(
            src_ref=src, dst_ref=dst, send_sem=send_sem, recv_sem=recv_sem,
            device_id=device, device_id_type=MESH)

    def kv_copies(peer):
        head = aligned(peer * KV // count, HD)
        mine = aligned(me, tok)
        return (remote(k_in.at[:, head], k_all.at[mine], k_sent.at[peer], kv_got.at[0],
                       (sec, peer)),
                remote(v_in.at[:, head], v_all.at[mine], v_sent.at[peer], kv_got.at[1],
                       (sec, peer)))

    def qo_copies(peer):
        cols = aligned(peer, feats)
        mine = aligned(core, tok)
        return (remote(q_in.at[:, cols], q_all.at[chip, mine], q_sent.at[peer],
                       q_got.at[chip], (sec, peer)),
                remote(o_in.at[:, cols], o_all.at[chip, mine], o_sent.at[peer],
                       o_got.at[chip], (sec, peer)))

    def w_copy():
        return remote(wq_in.at[:, aligned(1 - core, half)], weights.at[pl.ds(pl.multiple_of(core * span, HD), feats)],
                      w_sent.at[0], w_got.at[0], partner)

    def each_peer(act):
        for far in range(chips - 1, 0, -1):
            for p in range(2):
                @pl.when(chip + far < chips)
                def _():
                    act(2 * (chip + far) + p)

                @pl.when(chip >= far)
                def _():
                    act(2 * (chip - far) + p)
        act(me + 1 - 2 * core)

    def start_both(copies):
        for copy in copies:
            copy.start()

    each_peer(lambda peer: start_both(kv_copies(peer)))
    each_peer(lambda peer: start_both(qo_copies(peer)))
    w_copy().start()

    mine = aligned(me, tok)
    own = aligned(me * KV // count, HD)
    pltpu.make_async_copy(k_in.at[:, own], k_all.at[mine], kv_got.at[0]).start()
    pltpu.make_async_copy(v_in.at[:, own], v_all.at[mine], kv_got.at[1]).start()
    own = aligned(me, feats)
    mine = aligned(core, tok)
    pltpu.make_async_copy(q_in.at[:, own], q_all.at[chip, mine], q_got.at[chip]).start()
    pltpu.make_async_copy(o_in.at[:, own], o_all.at[chip, mine], o_got.at[chip]).start()

    my_half = aligned(core, half)
    my_rows = pl.ds(pl.multiple_of(core * span, HD), feats)
    local = [pltpu.make_async_copy(wq_in.at[:, my_half], weights.at[my_rows], w_local.at[0])]
    for p in range(2):
        g = aligned((2 * chip + p) * KV // count, HD)
        base = p * span + feats
        local.append(pltpu.make_async_copy(
            wk_in.at[g, my_half], weights.at[base:base + HD], w_local.at[1 + p]))
        local.append(pltpu.make_async_copy(
            wv_in.at[g, my_half], weights.at[base + HD:base + 2 * HD], w_local.at[3 + p]))
    for copy in local:
        copy.start()

    @pl.when(sec == sections - 1)
    def _():
        out_ref[...] = jnp.zeros_like(out_ref)

    dk_sum[...] = jnp.zeros_like(dk_sum)
    dv_sum[...] = jnp.zeros_like(dv_sum)

    pltpu.make_async_copy(k_all, k_all, kv_got.at[0]).wait()
    pltpu.make_async_copy(v_all, v_all, kv_got.at[1]).wait()
    k_turned[...] = k_all[...].T

    def grad_copy(b, p):
        here = grads.at[b * rows:(b + 1) * rows, pl.ds(pl.multiple_of(p * span, HD), span)]
        return remote(here, here, g_sent.at[b], g_got.at[b], partner)

    def attend(b):
        lo, hi = b * rows, (b + 1) * rows
        pltpu.make_async_copy(q_all.at[b], q_all.at[b], q_got.at[b]).wait()
        pltpu.make_async_copy(o_all.at[b], o_all.at[b], o_got.at[b]).wait()
        last = (((1,), (1,)), ((), ()))

        def one_head(h, carry):
            q = q_all[b, :, aligned(h, HD)]
            o = o_all[b, :, aligned(h, HD)]
            s = lax.dot_general(k_all[:hi], q, last, preferred_element_type=F32)
            dp = lax.dot_general(v_all[:hi], o, last, preferred_element_type=F32)
            j = lax.broadcasted_iota(jnp.int32, (hi, rows), 0)
            at = lax.broadcasted_iota(jnp.int32, (hi, rows), 1) + lo
            allowed = (j >= start_ref[:, lo:hi]) & (j <= at)
            s = jnp.where(allowed, s, -jnp.inf)
            top = jnp.max(s, axis=0, keepdims=True)
            e = jnp.exp2((s - top) * to_log2)
            inv = 1.0 / jnp.sum(e, axis=0, keepdims=True)
            delta = jnp.sum(e * dp, axis=0, keepdims=True) * inv
            p_low = (e * inv).astype(BF16)
            ds = (e * (dp - delta) * (inv * scale)).astype(BF16)
            dv_sum[:hi] += jnp.dot(p_low, o, preferred_element_type=F32)
            dk_sum[:hi] += jnp.dot(ds, q, preferred_element_type=F32)
            dq = jnp.dot(k_turned[:, :hi], ds, preferred_element_type=F32)
            col = pl.ds(pl.multiple_of(core * span + h * HD, HD), HD)
            grads[lo:hi, col] = dq.T.astype(BF16)
            return carry

        lax.fori_loop(0, heads, one_head, 0)
        tail = core * span + feats
        grads[lo:hi, pl.ds(pl.multiple_of(tail, HD), HD)] = dk_sum[lo:hi].astype(BF16)
        grads[lo:hi, pl.ds(pl.multiple_of(tail + HD, HD), HD)] = dv_sum[lo:hi].astype(BF16)
        grad_copy(b, core).start()

    def right_copy(d, k):
        here = right_buf.at[d, k]
        return remote(here, here, right_sent.at[d, k], right_got.at[d, k],
                      (sec, jnp.minimum(me + 2, count - 2 + core)))

    def left_copy(d, k):
        here = left_buf.at[d, k]
        return remote(here, here, left_sent.at[d, k], left_got.at[d, k],
                      (sec, jnp.maximum(me - 2, core)))

    def final_copy(k, p):
        return remote(final.at[k, p * tok:(p + 1) * tok],
                      out_ref.at[:, aligned(core * chunks + k, cw)],
                      final_sent.at[k, p], final_got.at[core, k],
                      (jnp.maximum(sec - 1, 0), 2 * chip + p))

    def product(d, k):
        return jnp.dot(grads[aligned(d, rows), :], weights[:, aligned(k, cw)],
                       preferred_element_type=F32)

    def set_out(d, buf, copy):
        def one(k, carry):
            buf[d, k] = product(d, k).astype(BF16)
            copy(d, k).start()
            return carry

        lax.fori_loop(0, chunks, one, 0)

    def pass_on(d, k, buf, copy):
        acc[...] = product(d, k)
        copy(d, k).wait_recv()
        buf[d, k] = (acc[...] + buf[d, k].astype(F32)).astype(BF16)
        copy(d, k).start()

    def finish(k):
        acc[...] = product(chip, k)

        @pl.when(chip > 0)
        def _():
            right_copy(chip, k).wait_recv()
            acc[...] += right_buf[chip, k].astype(F32)

        @pl.when(chip < chips - 1)
        def _():
            left_copy(chip, k).wait_recv()
            acc[...] += left_buf[chip, k].astype(F32)

        final[k] = acc[...].astype(BF16)

        @pl.when(sec > 0)
        def _():
            final_copy(k, 0).start()
            final_copy(k, 1).start()

    for b in range(chips - 1, -1, -1):
        attend(b)
        if b == chips - 1:
            for copy in local:
                copy.wait()
            other = pl.ds(pl.multiple_of((1 - core) * span, HD), feats)
            remote(wq_in.at[:, my_half], weights.at[other],
                   w_sent.at[0], w_got.at[0], partner).wait_recv()
        grad_copy(b, 1 - core).wait_recv()
        if b > 0:
            @pl.when(chip == 0)
            def _():
                set_out(b, right_buf, right_copy)
        if b < chips - 1:
            @pl.when(chip == chips - 1)
            def _():
                set_out(b, left_buf, left_copy)

    middle = (chip > 0) & (chip < chips - 1)

    @pl.when(chip > 0)
    def _():
        def one(i, carry):
            pass_on(chips - 1 - i // chunks, i % chunks, right_buf, right_copy)
            return carry

        lax.fori_loop(0, (chips - 1 - chip) * chunks, one, 0)

    def finish_one(k, carry):
        @pl.when(middle)
        def _():
            pass_on(chip - 1, k, left_buf, left_copy)

        finish(k)
        return carry

    lax.fori_loop(0, chunks, finish_one, 0)

    @pl.when(middle)
    def _():
        def one(i, carry):
            pass_on(chip - 2 - i // chunks, i % chunks, left_buf, left_copy)
            return carry

        lax.fori_loop(0, (chip - 1) * chunks, one, 0)

    def sent_both(copies):
        for copy in copies:
            copy.wait_send()

    each_peer(lambda peer: sent_both(kv_copies(peer)))
    each_peer(lambda peer: sent_both(qo_copies(peer)))
    for b in range(chips):
        grad_copy(b, core).wait_send()
    w_copy().wait_send()

    def drain(k, carry):
        def right_done(i, c):
            right_copy(chips - 1 - i, k).wait_send()
            return c

        def left_done(i, c):
            left_copy(i, k).wait_send()
            return c

        lax.fori_loop(0, chips - 1 - chip, right_done, 0)
        lax.fori_loop(0, chip, left_done, 0)

        @pl.when(sec > 0)
        def _():
            final_copy(k, 0).wait_send()
            final_copy(k, 1).wait_send()

        @pl.when(sec < sections - 1)
        def _():
            for p in range(2):
                remote(final.at[k, :tok], out_ref.at[:, aligned(p * chunks + k, cw)],
                       final_sent.at[k, p], final_got.at[p, k], partner).wait_recv()

        return carry

    lax.fori_loop(0, chunks, drain, 0)


def body(queries, keys, values, out_grad, documents, query_weight, key_weight, value_weight):
    sections = lax.axis_size("section")
    count = lax.axis_size("seq")
    tok = queries.shape[1]
    total = tok * count
    feats = query_weight.shape[1]
    heads = feats // HD
    width = query_weight.shape[2]
    chips = count // 2
    rows = 2 * tok
    cw = min(256, width // 2)
    chunks = width // 2 // cw
    ids = documents[0]
    start = jnp.sum((ids[:, None] < ids[None, :]).astype(jnp.int32), axis=0, keepdims=True)
    dma = pltpu.SemaphoreType.DMA
    deep = 2 * feats + 4 * HD
    anywhere = pl.BlockSpec(memory_space=pl.ANY)
    vmem = pl.BlockSpec(memory_space=pltpu.VMEM)
    out = pl.pallas_call(
        functools.partial(kernel, (sections, count, tok, heads, width, cw)),
        out_shape=jax.ShapeDtypeStruct((tok, width), BF16),
        in_specs=[anywhere] * 4 + [vmem] + [anywhere] * 3,
        out_specs=vmem,
        scratch_shapes=[
            pltpu.VMEM((chips, rows, feats), BF16),
            pltpu.VMEM((chips, rows, feats), BF16),
            pltpu.VMEM((total, HD), BF16),
            pltpu.VMEM((total, HD), BF16),
            pltpu.VMEM((HD, total), BF16),
            pltpu.VMEM((total, HD), F32),
            pltpu.VMEM((total, HD), F32),
            pltpu.VMEM((total, deep), BF16),
            pltpu.VMEM((deep, width // 2), BF16),
            pltpu.VMEM((chips, chunks, rows, cw), BF16),
            pltpu.VMEM((chips, chunks, rows, cw), BF16),
            pltpu.VMEM((rows, cw), F32),
            pltpu.VMEM((chunks, rows, cw), BF16),
            dma((count,)),
            dma((count,)),
            dma((count,)),
            dma((count,)),
            dma((chips,)),
            dma((chips,)),
            dma((2,)),
            dma((5,)),
            dma((1,)),
            dma((1,)),
            dma((chips,)),
            dma((chips,)),
            dma((chips, chunks)),
            dma((chips, chunks)),
            dma((chips, chunks)),
            dma((chips, chunks)),
            dma((chunks, 2)),
            dma((2, chunks)),
        ],
        compiler_params=pltpu.CompilerParams(
            collective_id=0, has_side_effects=True, vmem_limit_bytes=62 * 1024 * 1024),
        name="attention_back",
    )(queries[0], keys[0], values[0], out_grad[0], start,
      query_weight[0], key_weight[0], value_weight[0])
    return out[None]


def solution(mesh):
    in_specs = (
        P("section", "seq", None),
        P("section", "seq", None),
        P("section", "seq", None),
        P("section", "seq", None),
        P("section", None),
        P("section", "seq", None),
        P("section", None, None),
        P("section", None, None),
    )
    out_specs = P("section", "seq", None)
    return jax.shard_map(body, mesh=mesh, in_specs=in_specs, out_specs=out_specs, check_vma=False)
```

```python
import functools
import math

import jax
import jax.numpy as jnp
from jax import lax
from jax.experimental import pallas as pl
from jax.experimental.pallas import tpu as pltpu
from jax.sharding import PartitionSpec as P

KV = 4
HD = 128
MESH = pl.DeviceIdType.MESH
F32 = jnp.float32
BF16 = jnp.bfloat16


def aligned(index, size):
    return pl.ds(pl.multiple_of(index * size, size), size)


def kernel(dims, q_in, k_in, v_in, o_in, ids_ref, wq_in, wk_in, wv_in, out_ref,
           q_all, o_all, k_all, v_all, k_turned, dk_sum, dv_sum, start_ref, grads, weights,
           right_buf, left_buf, acc, final,
           q_sent, o_sent, k_sent, v_sent, q_got, o_got, kv_got, kv_forwarded,
           w_local, w_sent, w_got, g_sent, g_got,
           right_sent, right_got, left_sent, left_got, final_sent, final_got):
    sections, count, tok, heads, width, cw = dims
    total = tok * count
    chips = count // 2
    rows = 2 * tok
    feats = heads * HD
    span = feats + 2 * HD
    half = width // 2
    chunks = half // cw
    scale = 1.0 / math.sqrt(HD)
    to_log2 = scale * math.log2(math.e)
    sec = lax.axis_index("section")
    me = lax.axis_index("seq")
    chip = me // 2
    core = me % 2
    partner = (sec, me + 1 - 2 * core)

    barrier = pltpu.get_barrier_semaphore()

    def greet(device):
        pl.semaphore_signal(barrier, inc=1, device_id=device, device_id_type=MESH)

    for off in range(1, count):
        greet((sec, lax.rem(me + off, count)))
    for p in range(2):
        @pl.when(sec > 0)
        def _():
            greet((sec - 1, 2 * chip + p))

        @pl.when(sec < sections - 1)
        def _():
            greet((sec + 1, 2 * chip + p))
    above = jnp.where(sec > 0, 2, 0)
    below = jnp.where(sec < sections - 1, 2, 0)
    pl.semaphore_wait(barrier, count - 1 + above + below)

    def remote(src, dst, send_sem, recv_sem, device):
        return pltpu.make_async_remote_copy(
            src_ref=src, dst_ref=dst, send_sem=send_sem, recv_sem=recv_sem,
            device_id=device, device_id_type=MESH)

    def kv_copies(peer):
        head = aligned(peer * KV // count, HD)
        mine = aligned(me, tok)
        return (remote(k_in.at[:, head], k_all.at[mine], k_sent.at[peer], kv_got.at[0, me],
                       (sec, peer)),
                remote(v_in.at[:, head], v_all.at[mine], v_sent.at[peer], kv_got.at[1, me],
                       (sec, peer)))

    def qo_copies(peer):
        cols = aligned(peer, feats)
        mine = aligned(core, tok)
        return (remote(q_in.at[:, cols], q_all.at[chip, mine], q_sent.at[peer],
                       q_got.at[chip], (sec, peer)),
                remote(o_in.at[:, cols], o_all.at[chip, mine], o_sent.at[peer],
                       o_got.at[chip], (sec, peer)))

    def w_copy():
        return remote(wq_in.at[:, aligned(1 - core, half)], weights.at[pl.ds(pl.multiple_of(core * span, HD), feats)],
                      w_sent.at[0], w_got.at[0], partner)

    def each_twin(act):
        for far in range(chips - 1, 0, -1):
            @pl.when(chip + far < chips)
            def _():
                act(me + 2 * far)

            @pl.when(chip >= far)
            def _():
                act(me - 2 * far)
        act(me + 1 - 2 * core)

    def each_peer(act):
        for far in range(chips - 1, 0, -1):
            for p in range(2):
                @pl.when(chip + far < chips)
                def _():
                    act(2 * (chip + far) + p)

                @pl.when(chip >= far)
                def _():
                    act(2 * (chip - far) + p)
        act(me + 1 - 2 * core)

    def start_both(copies):
        for copy in copies:
            copy.start()

    each_twin(lambda peer: start_both(kv_copies(peer)))
    each_peer(lambda peer: start_both(qo_copies(peer)))
    w_copy().start()

    mine = aligned(me, tok)
    own = aligned(me * KV // count, HD)
    pltpu.make_async_copy(k_in.at[:, own], k_all.at[mine], kv_got.at[0, me]).start()
    pltpu.make_async_copy(v_in.at[:, own], v_all.at[mine], kv_got.at[1, me]).start()
    own = aligned(me, feats)
    mine = aligned(core, tok)
    pltpu.make_async_copy(q_in.at[:, own], q_all.at[chip, mine], q_got.at[chip]).start()
    pltpu.make_async_copy(o_in.at[:, own], o_all.at[chip, mine], o_got.at[chip]).start()

    my_half = aligned(core, half)
    my_rows = pl.ds(pl.multiple_of(core * span, HD), feats)
    local = [pltpu.make_async_copy(wq_in.at[:, my_half], weights.at[my_rows], w_local.at[0])]
    for p in range(2):
        g = aligned((2 * chip + p) * KV // count, HD)
        base = p * span + feats
        local.append(pltpu.make_async_copy(
            wk_in.at[g, my_half], weights.at[base:base + HD], w_local.at[1 + p]))
        local.append(pltpu.make_async_copy(
            wv_in.at[g, my_half], weights.at[base + HD:base + 2 * HD], w_local.at[3 + p]))
    for copy in local:
        copy.start()

    @pl.when(sec == sections - 1)
    def _():
        out_ref[...] = jnp.zeros_like(out_ref)

    dk_sum[...] = jnp.zeros_like(dk_sum)
    dv_sum[...] = jnp.zeros_like(dv_sum)

    turned = jnp.broadcast_to(ids_ref[...], (HD, total)).T[:, :1]
    for b in range(chips):
        before = turned < ids_ref[:, b * rows:(b + 1) * rows]
        start_ref[:, b * rows:(b + 1) * rows] = jnp.sum(
            before.astype(jnp.int32), axis=0, keepdims=True)

    def forward(which, b):
        buf = (k_all, v_all)[which]
        part = buf.at[aligned(2 * b + core, tok)]
        return remote(part, part, kv_forwarded.at[which, b], kv_got.at[which, 2 * b + core],
                      partner)

    def kv_wait(which, source):
        part = (k_all, v_all)[which].at[aligned(source, tok)]
        pltpu.make_async_copy(part, part, kv_got.at[which, source]).wait()

    for b in range(chips):
        for which in range(2):
            kv_wait(which, 2 * b + core)

            @pl.when(chip != b)
            def _():
                forward(which, b).start()
    for b in range(chips):
        for which in range(2):
            kv_wait(which, 2 * b + 1 - core)
    k_turned[...] = k_all[...].T

    def grad_copy(b, p):
        here = grads.at[b * rows:(b + 1) * rows, pl.ds(pl.multiple_of(p * span, HD), span)]
        return remote(here, here, g_sent.at[b], g_got.at[b], partner)

    def attend(b):
        lo, hi = b * rows, (b + 1) * rows
        pltpu.make_async_copy(q_all.at[b], q_all.at[b], q_got.at[b]).wait()
        pltpu.make_async_copy(o_all.at[b], o_all.at[b], o_got.at[b]).wait()
        last = (((1,), (1,)), ((), ()))

        def one_head(h, carry):
            q = q_all[b, :, aligned(h, HD)]
            o = o_all[b, :, aligned(h, HD)]
            s = lax.dot_general(k_all[:hi], q, last, preferred_element_type=F32)
            dp = lax.dot_general(v_all[:hi], o, last, preferred_element_type=F32)
            j = lax.broadcasted_iota(jnp.int32, (hi, rows), 0)
            at = lax.broadcasted_iota(jnp.int32, (hi, rows), 1) + lo
            allowed = (j >= start_ref[:, lo:hi]) & (j <= at)
            s = jnp.where(allowed, s, -jnp.inf)
            top = jnp.max(s, axis=0, keepdims=True)
            e = jnp.exp2((s - top) * to_log2)
            inv = 1.0 / jnp.sum(e, axis=0, keepdims=True)
            delta = jnp.sum(e * dp, axis=0, keepdims=True) * inv
            p_low = (e * inv).astype(BF16)
            ds = (e * (dp - delta) * (inv * scale)).astype(BF16)
            dv_sum[:hi] += jnp.dot(p_low, o, preferred_element_type=F32)
            dk_sum[:hi] += jnp.dot(ds, q, preferred_element_type=F32)
            dq = jnp.dot(k_turned[:, :hi], ds, preferred_element_type=F32)
            col = pl.ds(pl.multiple_of(core * span + h * HD, HD), HD)
            grads[lo:hi, col] = dq.T.astype(BF16)
            return carry

        lax.fori_loop(0, heads, one_head, 0)
        tail = core * span + feats
        grads[lo:hi, pl.ds(pl.multiple_of(tail, HD), HD)] = dk_sum[lo:hi].astype(BF16)
        grads[lo:hi, pl.ds(pl.multiple_of(tail + HD, HD), HD)] = dv_sum[lo:hi].astype(BF16)
        grad_copy(b, core).start()

    def right_copy(d, k):
        here = right_buf.at[d, k]
        return remote(here, here, right_sent.at[d, k], right_got.at[d, k],
                      (sec, jnp.minimum(me + 2, count - 2 + core)))

    def left_copy(d, k):
        here = left_buf.at[d, k]
        return remote(here, here, left_sent.at[d, k], left_got.at[d, k],
                      (sec, jnp.maximum(me - 2, core)))

    def final_copy(k, p):
        return remote(final.at[k, p * tok:(p + 1) * tok],
                      out_ref.at[:, aligned(core * chunks + k, cw)],
                      final_sent.at[k, p], final_got.at[core, k],
                      (jnp.maximum(sec - 1, 0), 2 * chip + p))

    def product(d, k):
        return jnp.dot(grads[aligned(d, rows), :], weights[:, aligned(k, cw)],
                       preferred_element_type=F32)

    def set_out(d, buf, copy, first=0, end=None):
        def one(k, carry):
            buf[d, k] = product(d, k).astype(BF16)
            copy(d, k).start()
            return carry

        lax.fori_loop(first, chunks if end is None else end, one, 0)

    def pass_on(d, k, buf, copy):
        acc[...] = product(d, k)
        copy(d, k).wait_recv()
        buf[d, k] = (acc[...] + buf[d, k].astype(F32)).astype(BF16)
        copy(d, k).start()

    def finish(k):
        acc[...] = product(chip, k)

        @pl.when(chip > 0)
        def _():
            right_copy(chip, k).wait_recv()
            acc[...] += right_buf[chip, k].astype(F32)

        @pl.when(chip < chips - 1)
        def _():
            left_copy(chip, k).wait_recv()
            acc[...] += left_buf[chip, k].astype(F32)

        final[k] = acc[...].astype(BF16)

        @pl.when(sec > 0)
        def _():
            final_copy(k, 0).start()
            final_copy(k, 1).start()

    early = chunks - chunks * 3 // 8
    for b in range(chips - 1, -1, -1):
        attend(b)
        if b == chips - 1:
            for copy in local:
                copy.wait()
            other = pl.ds(pl.multiple_of((1 - core) * span, HD), feats)
            remote(wq_in.at[:, my_half], weights.at[other],
                   w_sent.at[0], w_got.at[0], partner).wait_recv()
        grad_copy(b, 1 - core).wait_recv()
        if b > 0:
            @pl.when(chip == 0)
            def _():
                set_out(b, right_buf, right_copy)
        if b < chips - 1:
            @pl.when(chip == chips - 1)
            def _():
                set_out(b, left_buf, left_copy, 0, early if b == chips - 2 else chunks)

    @pl.when(chip == chips - 1)
    def _():
        set_out(chips - 2, left_buf, left_copy, early, chunks)

    middle = (chip > 0) & (chip < chips - 1)

    @pl.when(middle)
    def _():
        def to_right(i, carry):
            pass_on(chips - 1 - i // chunks, i % chunks, right_buf, right_copy)
            return carry

        def to_left(i, carry):
            pass_on(chip - 1 - i // chunks, i % chunks, left_buf, left_copy)
            return carry

        lax.fori_loop(0, (chip - 1) * chunks, to_left, 0)
        lax.fori_loop(0, (chips - 1 - chip) * chunks, to_right, 0)

    def finish_one(k, carry):
        @pl.when(middle)
        def _():
            pass_on(0, k, left_buf, left_copy)

        @pl.when((chip != chips - 2) | (k < early))
        def _():
            finish(k)

        return carry

    lax.fori_loop(0, chunks, finish_one, 0)

    @pl.when(chip == chips - 2)
    def _():
        def one(k, carry):
            finish(k)
            return carry

        lax.fori_loop(early, chunks, one, 0)

    def sent_both(copies):
        for copy in copies:
            copy.wait_send()

    each_twin(lambda peer: sent_both(kv_copies(peer)))
    for b in range(chips):
        @pl.when(chip != b)
        def _():
            forward(0, b).wait_send()
            forward(1, b).wait_send()
    each_peer(lambda peer: sent_both(qo_copies(peer)))
    for b in range(chips):
        grad_copy(b, core).wait_send()
    w_copy().wait_send()

    def drain(k, carry):
        def right_done(i, c):
            right_copy(chips - 1 - i, k).wait_send()
            return c

        def left_done(i, c):
            left_copy(i, k).wait_send()
            return c

        lax.fori_loop(0, chips - 1 - chip, right_done, 0)
        lax.fori_loop(0, chip, left_done, 0)

        @pl.when(sec > 0)
        def _():
            final_copy(k, 0).wait_send()
            final_copy(k, 1).wait_send()

        @pl.when(sec < sections - 1)
        def _():
            for p in range(2):
                remote(final.at[k, :tok], out_ref.at[:, aligned(p * chunks + k, cw)],
                       final_sent.at[k, p], final_got.at[p, k], partner).wait_recv()

        return carry

    lax.fori_loop(0, chunks, drain, 0)


def body(queries, keys, values, out_grad, documents, query_weight, key_weight, value_weight):
    sections = lax.axis_size("section")
    count = lax.axis_size("seq")
    tok = queries.shape[1]
    total = tok * count
    feats = query_weight.shape[1]
    heads = feats // HD
    width = query_weight.shape[2]
    chips = count // 2
    rows = 2 * tok
    cw = min(256, width // 2)
    chunks = width // 2 // cw
    dma = pltpu.SemaphoreType.DMA
    deep = 2 * feats + 4 * HD
    anywhere = pl.BlockSpec(memory_space=pl.ANY)
    vmem = pl.BlockSpec(memory_space=pltpu.VMEM)
    out = pl.pallas_call(
        functools.partial(kernel, (sections, count, tok, heads, width, cw)),
        out_shape=jax.ShapeDtypeStruct((tok, width), BF16),
        in_specs=[anywhere] * 4 + [vmem] + [anywhere] * 3,
        out_specs=vmem,
        scratch_shapes=[
            pltpu.VMEM((chips, rows, feats), BF16),
            pltpu.VMEM((chips, rows, feats), BF16),
            pltpu.VMEM((total, HD), BF16),
            pltpu.VMEM((total, HD), BF16),
            pltpu.VMEM((HD, total), BF16),
            pltpu.VMEM((total, HD), F32),
            pltpu.VMEM((total, HD), F32),
            pltpu.VMEM((1, total), jnp.int32),
            pltpu.VMEM((total, deep), BF16),
            pltpu.VMEM((deep, width // 2), BF16),
            pltpu.VMEM((chips, chunks, rows, cw), BF16),
            pltpu.VMEM((chips, chunks, rows, cw), BF16),
            pltpu.VMEM((rows, cw), F32),
            pltpu.VMEM((chunks, rows, cw), BF16),
            dma((count,)),
            dma((count,)),
            dma((count,)),
            dma((count,)),
            dma((chips,)),
            dma((chips,)),
            dma((2, count)),
            dma((2, chips)),
            dma((5,)),
            dma((1,)),
            dma((1,)),
            dma((chips,)),
            dma((chips,)),
            dma((chips, chunks)),
            dma((chips, chunks)),
            dma((chips, chunks)),
            dma((chips, chunks)),
            dma((chunks, 2)),
            dma((2, chunks)),
        ],
        compiler_params=pltpu.CompilerParams(
            collective_id=0, has_side_effects=True, vmem_limit_bytes=62 * 1024 * 1024),
        name="attention_back",
    )(queries[0], keys[0], values[0], out_grad[0], documents,
      query_weight[0], key_weight[0], value_weight[0])
    return out[None]


def solution(mesh):
    in_specs = (
        P("section", "seq", None),
        P("section", "seq", None),
        P("section", "seq", None),
        P("section", "seq", None),
        P("section", None),
        P("section", "seq", None),
        P("section", None, None),
        P("section", None, None),
    )
    out_specs = P("section", "seq", None)
    return jax.shard_map(body, mesh=mesh, in_specs=in_specs, out_specs=out_specs, check_vma=False)
```
